64 devices in a mesh: dp: 4 (over x, y), ep: 16 (over z, core).
Axes of the slice: x: 2, y: 2, z: 8, core: 2. Of those that a mesh axis runs over, the one named last changes fastest.
The devices are a block of a 4x4x8 slice.
Arguments:
- x_in: bfloat16 [192, 512, 768], P(('dp', 'ep')), parts along dimension 0
- pad_mask: int32 [192, 512], P(('dp', 'ep')), parts along dimension 0
- rel_bias: float32 [12, 512, 512], replicated
- expert_idx: int32 [2, 192, 512], P(None, ('dp', 'ep')), parts along dimension 1
- norm_scale: float32 [2, 2, 768], replicated
- w_query: bfloat16 [2, 768, 768], replicated
- w_key: bfloat16 [2, 768, 768], replicated
- w_value: bfloat16 [2, 768, 768], replicated
- w_attn_out: bfloat16 [2, 768, 768], replicated
- w_router: float32 [2, 768, 64], replicated
- w_in: bfloat16 [2, 64, 768, 3072], P(None, 'ep')
- w_out: bfloat16 [2, 64, 3072, 768], P(None, 'ep')
Outputs:
- output: bfloat16 [192, 512, 768], P(('dp', 'ep')), parts along dimension 0
There are 4 independent parts. The reference program is written for one: setup_inputs(seed, part) draws one part's arguments, and reference() takes and returns one part's arrays. A program takes and returns all parts, laid end to end along the dimension named above; an argument that names none is the same for every part.
All inputs are finite; a program needn't handle non-finite values.
Results may differ from the reference program's by a relative error of at most 0.0196086.
Values are sent between devices in bfloat16 or wider.
A program may use at most 768 MiB of HBM per device.

```python
import jax
import jax.numpy as jnp
from jax import lax

SEQS = 3
SEQ = 512
D = 768
HEADS = 12
HEAD = 64
FF = 3072
EXPERTS = 64
GROUPS = 16
CAP_FACTOR = 2
NORM_EPS = 1e-6
NEG_BIG = -1e9
TOKENS = SEQS * SEQ
NUM_SEQ = GROUPS * SEQS
INNER = HEADS * HEAD
CAPACITY = (CAP_FACTOR * TOKENS + EXPERTS - 1) // EXPERTS


def draw_mask(rng_key, num_seq):
    lengths = jax.random.randint(rng_key, (num_seq,), SEQ // 4, SEQ + 1)
    return (jnp.arange(SEQ)[None, :] < lengths[:, None]).astype(jnp.int32)


def draw_routes(rng_key, num_seq):
    route_keys = jax.random.split(rng_key, 5)
    rank_draws = [jax.random.randint(route_keys[draw_id], (2, num_seq, SEQ), 0, EXPERTS) for draw_id in range(3)]
    ranks = jnp.minimum(jnp.minimum(rank_draws[0], rank_draws[1]), rank_draws[2])
    perm_first = jax.random.permutation(route_keys[3], EXPERTS)
    perm_second = jax.random.permutation(route_keys[4], EXPERTS)
    return jnp.stack([perm_first[ranks[0]], perm_second[ranks[1]]]).astype(jnp.int32)


def setup_inputs(seed: int = 0, part: int = 0) -> dict:
    base_key = jax.random.key(seed)
    part_keys = jax.random.split(jax.random.fold_in(base_key, part), 3)
    shared_keys = jax.random.split(base_key, 10)
    x_in = jax.random.normal(part_keys[0], (NUM_SEQ, SEQ, D), jnp.float32).astype(jnp.bfloat16)
    pad_mask = draw_mask(part_keys[1], NUM_SEQ)
    expert_idx = draw_routes(part_keys[2], NUM_SEQ)
    rel_bias = 2.0 * jax.random.normal(shared_keys[0], (HEADS, SEQ, SEQ), jnp.float32)
    norm_scale = jax.random.uniform(shared_keys[1], (2, 2, D), jnp.float32, 0.5, 1.5)
    qk_std = (2.0 / D) ** 0.5 * HEAD ** -0.25
    w_query = (qk_std * jax.random.normal(shared_keys[2], (2, D, INNER), jnp.float32)).astype(jnp.bfloat16)
    w_key = (qk_std * jax.random.normal(shared_keys[3], (2, D, INNER), jnp.float32)).astype(jnp.bfloat16)
    w_value = (D ** -0.5 * jax.random.normal(shared_keys[4], (2, D, INNER), jnp.float32)).astype(jnp.bfloat16)
    w_attn_out = (INNER ** -0.5 * jax.random.normal(shared_keys[5], (2, INNER, D), jnp.float32)).astype(jnp.bfloat16)
    w_router = D ** -0.5 * jax.random.normal(shared_keys[6], (2, D, EXPERTS), jnp.float32)
    w_in = (D ** -0.5 * jax.random.normal(shared_keys[7], (2, EXPERTS, D, FF), jnp.float32)).astype(jnp.bfloat16)
    w_out = (EXPERTS * FF ** -0.5 * jax.random.normal(shared_keys[8], (2, EXPERTS, FF, D), jnp.float32)).astype(jnp.bfloat16)
    return dict(x_in=x_in, pad_mask=pad_mask, rel_bias=rel_bias, expert_idx=expert_idx, norm_scale=norm_scale, w_query=w_query, w_key=w_key, w_value=w_value, w_attn_out=w_attn_out, w_router=w_router, w_in=w_in, w_out=w_out)


def rms_norm(hidden, gain):
    hid32 = hidden.astype(jnp.float32)
    return hid32 * lax.rsqrt(jnp.mean(hid32 * hid32, axis=-1, keepdims=True) + NORM_EPS) * gain


def attention_block(hidden, pad_mask, rel_bias, gain, query_w, key_w, value_w, out_w):
    def one_sequence(seq_pair):
        seq_rows, seq_mask = seq_pair
        normed = rms_norm(seq_rows, gain).astype(jnp.bfloat16)
        query_rows = jnp.dot(normed, query_w, preferred_element_type=jnp.float32).astype(jnp.bfloat16).reshape(SEQ, HEADS, HEAD)
        key_rows = jnp.dot(normed, key_w, preferred_element_type=jnp.float32).astype(jnp.bfloat16).reshape(SEQ, HEADS, HEAD)
        value_rows = jnp.dot(normed, value_w, preferred_element_type=jnp.float32).astype(jnp.bfloat16).reshape(SEQ, HEADS, HEAD)
        scores = jnp.einsum('qhd,khd->hqk', query_rows.astype(jnp.float32), key_rows.astype(jnp.float32))
        scores = scores + rel_bias + jnp.where(seq_mask > 0, 0.0, NEG_BIG)[None, None, :]
        attn_probs = jax.nn.softmax(scores, axis=-1).astype(jnp.bfloat16)
        context = jnp.einsum('hqk,khd->qhd', attn_probs.astype(jnp.float32), value_rows.astype(jnp.float32))
        context = context.astype(jnp.bfloat16).reshape(SEQ, INNER)
        attn_out = jnp.dot(context, out_w, preferred_element_type=jnp.float32)
        return (seq_rows.astype(jnp.float32) + attn_out).astype(jnp.bfloat16)
    return lax.map(one_sequence, (hidden, pad_mask))


def expert_block(hidden, layer_ids, gain, route_w, up_w, down_w):
    grouped = hidden.reshape(GROUPS, TOKENS, D)
    ids_grouped = layer_ids.reshape(GROUPS, TOKENS)

    def route_group(grp_pair):
        grp_rows, grp_ids = grp_pair
        normed32 = rms_norm(grp_rows, gain)
        logits = jnp.dot(normed32, route_w, preferred_element_type=jnp.float32)
        gate_val = jnp.take_along_axis(jax.nn.softmax(logits, axis=-1), grp_ids[:, None], axis=1)[:, 0]
        one_hot = (grp_ids[:, None] == jnp.arange(EXPERTS)[None, :]).astype(jnp.int32)
        token_slot = jnp.take_along_axis(jnp.cumsum(one_hot, axis=0), grp_ids[:, None], axis=1)[:, 0] - 1
        flat_slot = jnp.where(token_slot < CAPACITY, grp_ids * CAPACITY + token_slot, EXPERTS * CAPACITY)
        slot_token = jnp.full((EXPERTS * CAPACITY,), TOKENS, jnp.int32).at[flat_slot].set(jnp.arange(TOKENS, dtype=jnp.int32), mode='drop')
        packed = jnp.take(normed32.astype(jnp.bfloat16), slot_token, axis=0, mode='fill', fill_value=0)
        return packed.reshape(EXPERTS, CAPACITY, D), gate_val, flat_slot

    packed, gate_val, flat_slot = lax.map(route_group, (grouped, ids_grouped))

    def one_expert(expert_parts):
        exp_rows, exp_up, exp_down = expert_parts
        flat_rows = exp_rows.reshape(GROUPS * CAPACITY, D)
        inner_act = jnp.maximum(jnp.dot(flat_rows, exp_up, preferred_element_type=jnp.float32), 0.0).astype(jnp.bfloat16)
        return jnp.dot(inner_act, exp_down, preferred_element_type=jnp.float32).astype(jnp.bfloat16).reshape(GROUPS, CAPACITY, D)

    expert_rows = lax.map(one_expert, (jnp.swapaxes(packed, 0, 1), up_w, down_w))
    expert_rows = jnp.swapaxes(expert_rows, 0, 1).reshape(GROUPS, EXPERTS * CAPACITY, D)

    def combine(grp_parts):
        grp_rows, grp_out, grp_gate, grp_flat = grp_parts
        returned = jnp.take(grp_out, grp_flat, axis=0, mode='fill', fill_value=0)
        return (grp_rows.astype(jnp.float32) + grp_gate[:, None] * returned.astype(jnp.float32)).astype(jnp.bfloat16)

    return lax.map(combine, (grouped, expert_rows, gate_val, flat_slot)).reshape(NUM_SEQ, SEQ, D)


def reference(x_in, pad_mask, rel_bias, expert_idx, norm_scale, w_query, w_key, w_value, w_attn_out, w_router, w_in, w_out):
    def layer_step(hidden, layer_params):
        gains, query_w, key_w, value_w, out_w, route_w, up_w, down_w, layer_ids = layer_params
        hidden = attention_block(hidden, pad_mask, rel_bias, gains[0], query_w, key_w, value_w, out_w)
        hidden = expert_block(hidden, layer_ids, gains[1], route_w, up_w, down_w)
        return hidden, None
    final_state = lax.scan(layer_step, x_in, (norm_scale, w_query, w_key, w_value, w_attn_out, w_router, w_in, w_out, expert_idx))
    return final_state[0]
```

```python
import functools

import jax
import jax.numpy as jnp
from jax import lax
from jax.experimental import pallas as pl
from jax.experimental.pallas import tpu as pltpu
from jax.sharding import PartitionSpec as P

NORM_EPS = 1e-6
NEG_BIG = -1e9
CAP_FACTOR = 2
LANES = 128
F32 = jnp.float32
BF16 = jnp.bfloat16


def rms(hid32, gain):
    return hid32 * lax.rsqrt(jnp.mean(hid32 * hid32, axis=-1, keepdims=True) + NORM_EPS) * gain


def slots_kernel(capacity, drop, e_ref, base_ref, pos_ref):
    layers, blocks, _ = e_ref.shape
    num_experts = base_ref.shape[1]
    row = lax.broadcasted_iota(jnp.int32, (LANES, LANES), 0)
    col = lax.broadcasted_iota(jnp.int32, (LANES, LANES), 1)
    upper = (row <= col).astype(F32).astype(BF16)
    experts = lax.broadcasted_iota(jnp.int32, (num_experts, LANES), 0)
    for layer in range(layers):
        carry = jnp.zeros((num_experts, 1), F32)
        for blk in range(blocks):
            hit = experts == e_ref[layer, blk:blk + 1, :]
            hot = hit.astype(F32)
            cum = jnp.dot(hot.astype(BF16), upper, preferred_element_type=F32) + (carry - 1.0)
            slot = jnp.sum(hot * cum, axis=0, keepdims=True)
            base = jnp.sum(hot * base_ref[0], axis=0, keepdims=True)
            carry = carry + jnp.sum(hot, axis=1, keepdims=True)
            pos_ref[layer, blk:blk + 1, :] = jnp.where(slot < capacity, base + slot, float(drop)).astype(jnp.int32)


def attn_kernel(head_dim, x_ref, mask_ref, bias_ref, g0_ref, g1_ref, wq_ref, wk_ref, wv_ref, wo_ref, wr_ref, e_ref,
                h1_ref, b_ref, gate_ref, q_s, k_s, v_s, ctx_s):
    pair = pl.program_id(0)
    seq = pl.program_id(1)
    pairs = pl.num_programs(0)
    n_pairs, width = q_s.shape[0], q_s.shape[3]

    @pl.when(pair == 0)
    def _():
        a = rms(x_ref[seq].astype(F32), g0_ref[...]).astype(BF16)
        for w_ref, dst in ((wq_ref, q_s), (wk_ref, k_s), (wv_ref, v_s)):
            rows = jnp.dot(a, w_ref[...], preferred_element_type=F32).astype(BF16)
            for j in range(n_pairs):
                dst[j, seq] = rows[:, j * width:(j + 1) * width]

    q2, k2, v2 = q_s[pair, seq], k_s[pair, seq], v_s[pair, seq]
    lane = lax.broadcasted_iota(jnp.int32, q2.shape, 1)
    mask_row = jnp.where(mask_ref[seq] > 0, 0.0, NEG_BIG)
    parts = []
    for half in range(width // head_dim):
        mine = (lane >= half * head_dim) & (lane < (half + 1) * head_dim)
        qh = jnp.where(mine, q2, jnp.zeros_like(q2))
        s = lax.dot_general(qh, k2, (((1,), (1,)), ((), ())), preferred_element_type=F32)
        s = s + bias_ref[half] + mask_row
        p = jnp.exp(s - jnp.max(s, axis=-1, keepdims=True))
        p = (p * (1.0 / jnp.sum(p, axis=-1, keepdims=True))).astype(BF16)
        o = jnp.dot(p, v2, preferred_element_type=F32)
        parts.append(jnp.where(mine, o, 0.0))
    ctx_s[seq, :, pl.ds(pl.multiple_of(pair * width, width), width)] = sum(parts).astype(BF16)

    @pl.when(pair == pairs - 1)
    def _():
        o = jnp.dot(ctx_s[seq], wo_ref[...], preferred_element_type=F32)
        h1 = (x_ref[seq].astype(F32) + o).astype(BF16)
        h1_ref[seq] = h1
        r = rms(h1.astype(F32), g1_ref[...])
        b_ref[seq] = r.astype(BF16)
        logits = jnp.dot(r, wr_ref[...], precision=lax.Precision.HIGHEST, preferred_element_type=F32)
        ex = jnp.exp(logits - jnp.max(logits, axis=-1, keepdims=True))
        chosen = lax.broadcasted_iota(jnp.int32, logits.shape, 1) == e_ref[seq]
        gate_ref[seq] = jnp.sum(jnp.where(chosen, ex, 0.0), axis=-1, keepdims=True) / jnp.sum(ex, axis=-1, keepdims=True)


def attention(layer, x, mask, rel_bias, gains, wq, wk, wv, wo, wr, e_col):
    num_seqs, seq_len, model_dim = x.shape
    num_heads = rel_bias.shape[0]
    inner = wq.shape[2]
    head_dim = inner // num_heads
    per = LANES // head_dim
    pairs = num_heads // per
    num_experts = wr.shape[2]
    full = lambda *shape: pl.BlockSpec(shape, lambda p, s: (0,) * len(shape))
    of_layer = lambda *shape: pl.BlockSpec((None,) + shape, lambda p, s: (layer,) + (0,) * len(shape))
    gain = lambda which: pl.BlockSpec((None, 1, model_dim), lambda p, s: (2 * layer + which, 0, 0))
    flops = 2 * num_seqs * seq_len * (4 * model_dim * inner + 2 * seq_len * inner)
    return pl.pallas_call(
        functools.partial(attn_kernel, head_dim),
        grid=(pairs, num_seqs),
        in_specs=[full(num_seqs, seq_len, model_dim), full(num_seqs, 1, seq_len),
                  pl.BlockSpec((per, seq_len, seq_len), lambda p, s: (p, 0, 0)), gain(0), gain(1),
                  of_layer(model_dim, inner), of_layer(model_dim, inner), of_layer(model_dim, inner),
                  of_layer(inner, model_dim), of_layer(model_dim, num_experts), of_layer(num_seqs, seq_len, 1)],
        out_specs=[full(num_seqs, seq_len, model_dim), full(num_seqs, seq_len, model_dim), full(num_seqs, seq_len, 1)],
        out_shape=[jax.ShapeDtypeStruct(x.shape, BF16), jax.ShapeDtypeStruct(x.shape, BF16),
                   jax.ShapeDtypeStruct((num_seqs, seq_len, 1), F32)],
        scratch_shapes=[pltpu.VMEM((pairs, num_seqs, seq_len, LANES), BF16)] * 3
        + [pltpu.VMEM((num_seqs, seq_len, inner), BF16)],
        compiler_params=pltpu.CompilerParams(dimension_semantics=("arbitrary", "arbitrary"), vmem_limit_bytes=60 << 20),
        cost_estimate=pl.CostEstimate(flops=flops, bytes_accessed=32 << 20, transcendentals=num_seqs * num_heads * seq_len * seq_len),
        name="attn",
    )(x, mask, rel_bias, gains, gains, wq, wk, wv, wo, wr, e_col)


def pack_kernel(pos_ref, b_ref, out_ref):
    rows, _ = out_ref.shape
    first = pl.program_id(0) * rows
    acc = None
    for blk in range(b_ref.shape[0]):
        want = lax.broadcasted_iota(jnp.int32, (rows, b_ref.shape[1]), 0) + first
        hot = (want == pos_ref[blk]).astype(F32).astype(BF16)
        part = jnp.dot(hot, b_ref[blk], preferred_element_type=F32)
        acc = part if acc is None else acc + part
    out_ref[...] = acc.astype(BF16)


def pack(layer, pos_row, b, slots, rows=256):
    num_seqs, seq_len, model_dim = b.shape
    return pl.pallas_call(
        pack_kernel,
        grid=(slots // rows,),
        in_specs=[pl.BlockSpec((None, num_seqs, 1, seq_len), lambda i: (layer, 0, 0, 0)),
                  pl.BlockSpec((num_seqs, seq_len, model_dim), lambda i: (0, 0, 0))],
        out_specs=pl.BlockSpec((rows, model_dim), lambda i: (i, 0)),
        out_shape=jax.ShapeDtypeStruct((slots, model_dim), BF16),
        compiler_params=pltpu.CompilerParams(dimension_semantics=("arbitrary",), vmem_limit_bytes=60 << 20),
        cost_estimate=pl.CostEstimate(flops=2 * slots * num_seqs * seq_len * model_dim, bytes_accessed=8 << 20, transcendentals=0),
        name="pack",
    )(pos_row, b)


def combine_kernel(pos_ref, gate_ref, h1_ref, u_ref, out_ref):
    hot = lax.broadcasted_iota(jnp.int32, (h1_ref.shape[0], u_ref.shape[0]), 1) == pos_ref[...]
    u = jnp.dot(hot.astype(F32).astype(BF16), u_ref[...], preferred_element_type=F32)
    out_ref[...] = (h1_ref[...].astype(F32) + gate_ref[...] * u).astype(BF16)


def combine(layer, pos_col, gate, h1, u, rows=256):
    num_seqs, seq_len, model_dim = h1.shape
    slots = u.shape[0]
    tok = lambda last: pl.BlockSpec((None, rows, last), lambda s, i: (s, i, 0))
    return pl.pallas_call(
        combine_kernel,
        grid=(num_seqs, seq_len // rows),
        in_specs=[pl.BlockSpec((None, None, rows, 1), lambda s, i: (layer, s, i, 0)), tok(1), tok(model_dim),
                  pl.BlockSpec((slots, model_dim), lambda s, i: (0, 0))],
        out_specs=tok(model_dim),
        out_shape=jax.ShapeDtypeStruct(h1.shape, BF16),
        compiler_params=pltpu.CompilerParams(dimension_semantics=("arbitrary", "arbitrary"), vmem_limit_bytes=60 << 20),
        cost_estimate=pl.CostEstimate(flops=2 * slots * num_seqs * seq_len * model_dim, bytes_accessed=10 << 20, transcendentals=0),
        name="combine",
    )(pos_col, gate, h1, u)


def ffn_kernel(x_ref, w_in_ref, w_out_ref, y_ref, acc_ref):
    part = pl.program_id(1)
    act = jnp.maximum(jnp.dot(x_ref[...], w_in_ref[...], preferred_element_type=F32), 0.0).astype(BF16)
    down = jnp.dot(act, w_out_ref[...], preferred_element_type=F32)

    @pl.when(part == 0)
    def _():
        acc_ref[...] = down

    @pl.when((part > 0) & (part < pl.num_programs(1) - 1))
    def _():
        acc_ref[...] += down

    @pl.when(part == pl.num_programs(1) - 1)
    def _():
        y_ref[...] = (acc_ref[...] + down).astype(BF16)


def expert_ffn(layer, x, w_in, w_out, cols=768):
    mine, rows, model_dim = x.shape
    ff = w_in.shape[3]
    return pl.pallas_call(
        ffn_kernel,
        grid=(mine, ff // cols),
        in_specs=[pl.BlockSpec((None, rows, model_dim), lambda e, f: (e, 0, 0)),
                  pl.BlockSpec((None, None, model_dim, cols), lambda e, f: (layer, e, 0, f)),
                  pl.BlockSpec((None, None, cols, model_dim), lambda e, f: (layer, e, f, 0))],
        out_specs=pl.BlockSpec((None, rows, model_dim), lambda e, f: (e, 0, 0)),
        out_shape=jax.ShapeDtypeStruct(x.shape, BF16),
        scratch_shapes=[pltpu.VMEM((rows, model_dim), F32)],
        compiler_params=pltpu.CompilerParams(dimension_semantics=("arbitrary", "arbitrary"), vmem_limit_bytes=60 << 20),
        cost_estimate=pl.CostEstimate(flops=4 * mine * rows * model_dim * ff, bytes_accessed=48 << 20, transcendentals=0),
        name="ffn",
    )(x, w_in, w_out)


def solution(mesh):
    token_spec = P(('dp', 'ep'))
    peers = mesh.shape['ep']

    def per_device(x_in, pad_mask, rel_bias, expert_idx, norm_scale, w_query, w_key, w_value, w_attn_out, w_router, w_in, w_out):
        num_seqs, seq_len, model_dim = x_in.shape
        tok_count = num_seqs * seq_len
        layers = w_router.shape[0]
        num_experts = w_router.shape[2]
        mine = num_experts // peers
        capacity = (CAP_FACTOR * tok_count + num_experts - 1) // num_experts
        slots = num_experts * capacity
        expert_ids = jnp.arange(num_experts, dtype=jnp.int32)
        base = ((expert_ids % mine) * (peers * capacity) + (expert_ids // mine) * capacity).astype(F32)
        blocks = expert_idx.reshape(layers, tok_count // LANES, LANES)
        pos = pl.pallas_call(
            functools.partial(slots_kernel, capacity, slots),
            out_shape=jax.ShapeDtypeStruct(blocks.shape, jnp.int32),
            name="slots",
        )(blocks, base.reshape(1, num_experts, 1))
        pos_row = pos.reshape(layers, num_seqs, 1, seq_len)
        pos_col = pos.reshape(layers, num_seqs, seq_len, 1)
        e_col = expert_idx.reshape(layers, num_seqs, seq_len, 1)
        mask = pad_mask.reshape(num_seqs, 1, seq_len)
        gains = norm_scale.reshape(layers * 2, 1, model_dim)
        hidden = x_in
        for layer in range(layers):
            h1, b, gate = attention(layer, hidden, mask, rel_bias, gains, w_query, w_key, w_value, w_attn_out, w_router, e_col)
            packed = pack(layer, pos_row, b, slots)
            received = lax.all_to_all(packed.reshape(mine, peers, capacity, model_dim), 'ep', 1, 1, tiled=True)
            rows = expert_ffn(layer, received.reshape(mine, peers * capacity, model_dim), w_in, w_out)
            returned = lax.all_to_all(rows.reshape(mine, peers, capacity, model_dim), 'ep', 1, 1, tiled=True)
            hidden = combine(layer, pos_col, gate, h1, returned.reshape(slots, model_dim))
        return hidden

    return jax.shard_map(per_device, mesh=mesh, in_specs=(token_spec, token_spec, P(), P(None, ('dp', 'ep')), P(), P(), P(), P(), P(), P(), P(None, 'ep'), P(None, 'ep')), out_specs=token_spec, check_vma=False)
```

```python
import functools

import jax
import jax.numpy as jnp
from jax import lax
from jax.experimental import pallas as pl
from jax.experimental.pallas import tpu as pltpu
from jax.sharding import PartitionSpec as P

NORM_EPS = 1e-6
NEG_BIG = -1e9
CAP_FACTOR = 2
LANES = 128
F32 = jnp.float32
BF16 = jnp.bfloat16


def rms(hid32, gain):
    return hid32 * lax.rsqrt(jnp.mean(hid32 * hid32, axis=-1, keepdims=True) + NORM_EPS) * gain


def slots_kernel(capacity, drop, e_ref, base_ref, pos_ref):
    layers, blocks, _ = e_ref.shape
    num_experts = base_ref.shape[1]
    row = lax.broadcasted_iota(jnp.int32, (LANES, LANES), 0)
    col = lax.broadcasted_iota(jnp.int32, (LANES, LANES), 1)
    upper = (row <= col).astype(F32).astype(BF16)
    experts = lax.broadcasted_iota(jnp.int32, (num_experts, LANES), 0)
    for layer in range(layers):
        carry = jnp.zeros((num_experts, 1), F32)
        for blk in range(blocks):
            hit = experts == e_ref[layer, blk:blk + 1, :]
            hot = hit.astype(F32)
            cum = jnp.dot(hot.astype(BF16), upper, preferred_element_type=F32) + (carry - 1.0)
            slot = jnp.sum(hot * cum, axis=0, keepdims=True)
            base = jnp.sum(hot * base_ref[0], axis=0, keepdims=True)
            carry = carry + jnp.sum(hot, axis=1, keepdims=True)
            pos_ref[layer, blk:blk + 1, :] = jnp.where(slot < capacity, base + slot, float(drop)).astype(jnp.int32)


def attn_kernel(head_dim, x_ref, mask_ref, bias_ref, g0_ref, g1_ref, wq_ref, wk_ref, wv_ref, wo_ref, wr_ref, e_ref,
                h1_ref, b_ref, gate_ref, q_s, k_s, v_s, ctx_s):
    pair = pl.program_id(0)
    seq = pl.program_id(1)
    pairs = pl.num_programs(0)
    n_pairs, width = q_s.shape[0], q_s.shape[3]

    @pl.when(pair == 0)
    def _():
        a = rms(x_ref[seq].astype(F32), g0_ref[...]).astype(BF16)
        for w_ref, dst in ((wq_ref, q_s), (wk_ref, k_s), (wv_ref, v_s)):
            rows = jnp.dot(a, w_ref[...], preferred_element_type=F32).astype(BF16)
            for j in range(n_pairs):
                dst[j, seq] = rows[:, j * width:(j + 1) * width]

    q2, k2, v2 = q_s[pair, seq], k_s[pair, seq], v_s[pair, seq]
    lane = lax.broadcasted_iota(jnp.int32, q2.shape, 1)
    mask_row = jnp.where(mask_ref[seq] > 0, 0.0, NEG_BIG)
    parts = []
    for half in range(width // head_dim):
        mine = (lane >= half * head_dim) & (lane < (half + 1) * head_dim)
        qh = jnp.where(mine, q2, jnp.zeros_like(q2))
        s = lax.dot_general(qh, k2, (((1,), (1,)), ((), ())), preferred_element_type=F32)
        s = s + bias_ref[half] + mask_row
        p = jnp.exp(s - jnp.max(s, axis=-1, keepdims=True))
        p = (p * (1.0 / jnp.sum(p, axis=-1, keepdims=True))).astype(BF16)
        o = jnp.dot(p, v2, preferred_element_type=F32)
        parts.append(jnp.where(mine, o, 0.0))
    ctx_s[seq, :, pl.ds(pl.multiple_of(pair * width, width), width)] = sum(parts).astype(BF16)

    @pl.when(pair == pairs - 1)
    def _():
        o = jnp.dot(ctx_s[seq], wo_ref[...], preferred_element_type=F32)
        h1 = (x_ref[seq].astype(F32) + o).astype(BF16)
        h1_ref[seq] = h1
        r = rms(h1.astype(F32), g1_ref[...])
        b_ref[seq] = r.astype(BF16)
        logits = jnp.dot(r, wr_ref[...], precision=lax.Precision.HIGHEST, preferred_element_type=F32)
        ex = jnp.exp(logits - jnp.max(logits, axis=-1, keepdims=True))
        chosen = lax.broadcasted_iota(jnp.int32, logits.shape, 1) == e_ref[seq]
        gate_ref[seq] = jnp.sum(jnp.where(chosen, ex, 0.0), axis=-1, keepdims=True) / jnp.sum(ex, axis=-1, keepdims=True)


def attention(layer, x, mask, rel_bias, gains, wq, wk, wv, wo, wr, e_col):
    num_seqs, seq_len, model_dim = x.shape
    num_heads = rel_bias.shape[0]
    inner = wq.shape[2]
    head_dim = inner // num_heads
    per = LANES // head_dim
    pairs = num_heads // per
    num_experts = wr.shape[2]
    full = lambda *shape: pl.BlockSpec(shape, lambda p, s: (0,) * len(shape))
    of_layer = lambda *shape: pl.BlockSpec((None,) + shape, lambda p, s: (layer,) + (0,) * len(shape))
    gain = lambda which: pl.BlockSpec((None, 1, model_dim), lambda p, s: (2 * layer + which, 0, 0))
    flops = 2 * num_seqs * seq_len * (4 * model_dim * inner + 2 * seq_len * inner)
    return pl.pallas_call(
        functools.partial(attn_kernel, head_dim),
        grid=(pairs, num_seqs),
        in_specs=[full(num_seqs, seq_len, model_dim), full(num_seqs, 1, seq_len),
                  pl.BlockSpec((per, seq_len, seq_len), lambda p, s: (p, 0, 0)), gain(0), gain(1),
                  of_layer(model_dim, inner), of_layer(model_dim, inner), of_layer(model_dim, inner),
                  of_layer(inner, model_dim), of_layer(model_dim, num_experts), of_layer(num_seqs, seq_len, 1)],
        out_specs=[full(num_seqs, seq_len, model_dim), full(num_seqs, seq_len, model_dim), full(num_seqs, seq_len, 1)],
        out_shape=[jax.ShapeDtypeStruct(x.shape, BF16), jax.ShapeDtypeStruct(x.shape, BF16),
                   jax.ShapeDtypeStruct((num_seqs, seq_len, 1), F32)],
        scratch_shapes=[pltpu.VMEM((pairs, num_seqs, seq_len, LANES), BF16)] * 3
        + [pltpu.VMEM((num_seqs, seq_len, inner), BF16)],
        compiler_params=pltpu.CompilerParams(dimension_semantics=("arbitrary", "arbitrary"), vmem_limit_bytes=60 << 20),
        cost_estimate=pl.CostEstimate(flops=flops, bytes_accessed=32 << 20, transcendentals=num_seqs * num_heads * seq_len * seq_len),
        name="attn",
    )(x, mask, rel_bias, gains, gains, wq, wk, wv, wo, wr, e_col)


def moe_kernel(layer, axis, pos_row_ref, pos_col_ref, gate_ref, h1_ref, b_ref, w_in_ref, w_out_ref, out_ref,
               packed, recv, ret, w_in_buf, w_out_buf, acc, u_acc, out_send, out_recv, back_send, back_recv, w_sem):
    mine, peers, capacity, dim = packed.shape
    num_seqs, seq_len, _ = b_ref.shape
    ff = w_in_buf.shape[2]
    rows = peers * capacity
    me = lax.axis_index(axis)
    other = lambda shift: lax.rem(me + shift, peers)

    def weights(k):
        slot = lax.rem(k, 2)
        return (pltpu.make_async_copy(w_in_ref.at[layer, k], w_in_buf.at[slot], w_sem.at[0, slot]),
                pltpu.make_async_copy(w_out_ref.at[layer, k], w_out_buf.at[slot], w_sem.at[1, slot]))

    def there(k, peer, slot):
        return pltpu.make_async_remote_copy(
            src_ref=packed.at[k, peer], dst_ref=recv.at[k, slot], send_sem=out_send.at[k, peer],
            recv_sem=out_recv.at[k, slot], device_id={axis: peer}, device_id_type=pl.DeviceIdType.MESH)

    def back(k, peer, slot):
        return pltpu.make_async_remote_copy(
            src_ref=recv.at[k, peer], dst_ref=ret.at[k, slot], send_sem=back_send.at[k, peer],
            recv_sem=back_recv.at[k, slot], device_id={axis: peer}, device_id_type=pl.DeviceIdType.MESH)

    def each_peer(fn):
        @pl.loop(1, peers)
        def _(shift):
            fn(other(shift))

    for k in range(min(2, mine)):
        for copy in weights(k):
            copy.start()

    barrier = pltpu.get_barrier_semaphore()
    each_peer(lambda peer: pl.semaphore_signal(barrier, inc=1, device_id={axis: peer}, device_id_type=pl.DeviceIdType.MESH))
    pl.semaphore_wait(barrier, peers - 1)

    half = peers // 2
    @pl.loop(0, mine)
    def _(k):
        @pl.loop(0, 2)
        def _(part):
            first = k * rows + part * (half * capacity)
            want = lax.broadcasted_iota(jnp.int32, (half * capacity, seq_len), 0) + first
            total = None
            for s in range(num_seqs):
                hot = (want == pos_row_ref[layer, s]).astype(F32).astype(BF16)
                term = jnp.dot(hot, b_ref[s], preferred_element_type=F32)
                total = term if total is None else total + term
            packed[k, pl.ds(part * half, half)] = total.astype(BF16).reshape(half, capacity, dim)
        each_peer(lambda peer: there(k, peer, me).start())
        recv[k, me] = packed[k, me]

    u_acc[...] = jnp.zeros_like(u_acc)

    @pl.loop(0, mine)
    def _(k):
        slot = lax.rem(k, 2)
        for copy in weights(k):
            copy.wait()
        each_peer(lambda peer: there(k, peer, peer).wait_recv())
        acc[...] = jnp.zeros_like(acc)

        @pl.loop(0, ff // dim)
        def _(part):
            cols = pl.ds(pl.multiple_of(part * dim, dim), dim)
            act = jnp.dot(recv[k].reshape(rows, dim), w_in_buf[slot, :, cols], preferred_element_type=F32)
            act = jnp.maximum(act, 0.0).astype(BF16)
            acc[...] += jnp.dot(act, w_out_buf[slot, cols, :], preferred_element_type=F32)

        recv[k] = acc[...].astype(BF16).reshape(peers, capacity, dim)
        each_peer(lambda peer: back(k, peer, me).start())
        ret[k, me] = recv[k, me]

        @pl.when(k + 2 < mine)
        def _():
            for copy in weights(k + 2):
                copy.start()

    def gather_back(k, last):
        each_peer(lambda peer: back(k, peer, peer).wait_recv())
        for s in range(num_seqs):
            @pl.loop(0, seq_len // 256)
            def _(part):
                tok = pl.ds(pl.multiple_of(part * 256, 256), 256)
                want = lax.broadcasted_iota(jnp.int32, (256, rows), 1) + k * rows
                hot = (want == pos_col_ref[layer, s, tok, :]).astype(F32).astype(BF16)
                u = jnp.dot(hot, ret[k].reshape(rows, dim), preferred_element_type=F32) + u_acc[s, tok, :].astype(F32)
                if last:
                    out_ref[s, tok, :] = (h1_ref[s, tok, :].astype(F32) + gate_ref[s, tok, :] * u).astype(BF16)
                else:
                    u_acc[s, tok, :] = u.astype(BF16)

    @pl.loop(0, mine - 1)
    def _(k):
        gather_back(k, False)

    gather_back(mine - 1, True)

    @pl.loop(0, mine)
    def _(k):
        each_peer(lambda peer: there(k, peer, me).wait_send())
        each_peer(lambda peer: back(k, peer, me).wait_send())


def moe(layer, axis, peers, capacity, pos_row, pos_col, gate, h1, b, w_in, w_out):
    num_seqs, seq_len, dim = h1.shape
    mine, _, ff = w_in.shape[1:]
    rows = peers * capacity
    near = pl.BlockSpec(memory_space=pltpu.VMEM)
    hbm = pl.BlockSpec(memory_space=pl.ANY)
    buffer = pltpu.VMEM((mine, peers, capacity, dim), BF16)
    sems = pltpu.SemaphoreType.DMA((mine, peers))
    return pl.pallas_call(
        functools.partial(moe_kernel, layer, axis),
        in_specs=[near] * 5 + [hbm, hbm],
        out_specs=near,
        out_shape=jax.ShapeDtypeStruct(h1.shape, BF16),
        scratch_shapes=[buffer, buffer, buffer, pltpu.VMEM((2, dim, ff), BF16), pltpu.VMEM((2, ff, dim), BF16),
                        pltpu.VMEM((rows, dim), F32), pltpu.VMEM((num_seqs, seq_len, dim), BF16),
                        sems, sems, sems, sems, pltpu.SemaphoreType.DMA((2, 2))],
        compiler_params=pltpu.CompilerParams(collective_id=layer, has_side_effects=True, vmem_limit_bytes=67043328),
        cost_estimate=pl.CostEstimate(flops=4 * mine * rows * dim * ff, bytes_accessed=48 << 20, transcendentals=0),
        name="moe",
    )(pos_row, pos_col, gate, h1, b, w_in, w_out)


def solution(mesh):
    token_spec = P(('dp', 'ep'))
    peers = mesh.shape['ep']

    def per_device(x_in, pad_mask, rel_bias, expert_idx, norm_scale, w_query, w_key, w_value, w_attn_out, w_router, w_in, w_out):
        num_seqs, seq_len, model_dim = x_in.shape
        tok_count = num_seqs * seq_len
        layers = w_router.shape[0]
        num_experts = w_router.shape[2]
        mine = num_experts // peers
        capacity = (CAP_FACTOR * tok_count + num_experts - 1) // num_experts
        slots = num_experts * capacity
        expert_ids = jnp.arange(num_experts, dtype=jnp.int32)
        base = ((expert_ids % mine) * (peers * capacity) + (expert_ids // mine) * capacity).astype(F32)
        blocks = expert_idx.reshape(layers, tok_count // LANES, LANES)
        pos = pl.pallas_call(
            functools.partial(slots_kernel, capacity, slots),
            out_shape=jax.ShapeDtypeStruct(blocks.shape, jnp.int32),
            name="slots",
        )(blocks, base.reshape(1, num_experts, 1))
        pos_row = pos.reshape(layers, num_seqs, 1, seq_len)
        pos_col = pos.reshape(layers, num_seqs, seq_len, 1)
        e_col = expert_idx.reshape(layers, num_seqs, seq_len, 1)
        mask = pad_mask.reshape(num_seqs, 1, seq_len)
        gains = norm_scale.reshape(layers * 2, 1, model_dim)
        hidden = x_in
        for layer in range(layers):
            h1, b, gate = attention(layer, hidden, mask, rel_bias, gains, w_query, w_key, w_value, w_attn_out, w_router, e_col)
            hidden = moe(layer, 'ep', peers, capacity, pos_row, pos_col, gate, h1, b, w_in, w_out)
        return hidden

    return jax.shard_map(per_device, mesh=mesh, in_specs=(token_spec, token_spec, P(), P(None, ('dp', 'ep')), P(), P(), P(), P(), P(), P(), P(None, 'ep'), P(None, 'ep')), out_specs=token_spec, check_vma=False)
```

```python
import functools

import jax
import jax.numpy as jnp
from jax import lax
from jax.experimental import pallas as pl
from jax.experimental.pallas import tpu as pltpu
from jax.sharding import PartitionSpec as P

NORM_EPS = 1e-6
NEG_BIG = -1e9
CAP_FACTOR = 2
LANES = 128
F32 = jnp.float32
BF16 = jnp.bfloat16


def rms(hid32, gain):
    return hid32 * lax.rsqrt(jnp.mean(hid32 * hid32, axis=-1, keepdims=True) + NORM_EPS) * gain


def slots_kernel(capacity, drop, e_ref, base_ref, pos_ref):
    layers, num_seqs, seq_len = e_ref.shape
    num_experts = base_ref.shape[1]
    row = lax.broadcasted_iota(jnp.int32, (LANES, LANES), 0)
    col = lax.broadcasted_iota(jnp.int32, (LANES, LANES), 1)
    upper = (row <= col).astype(F32).astype(BF16)
    experts = lax.broadcasted_iota(jnp.int32, (num_experts, LANES), 0)
    for layer in range(layers):
        carry = jnp.zeros((num_experts, 1), F32)
        for blk in range(num_seqs * seq_len // LANES):
            seq, first = divmod(blk * LANES, seq_len)
            hit = experts == e_ref[layer, seq:seq + 1, first:first + LANES]
            hot = hit.astype(F32)
            cum = jnp.dot(hot.astype(BF16), upper, preferred_element_type=F32) + (carry - 1.0)
            slot = jnp.sum(hot * cum, axis=0, keepdims=True)
            base = jnp.sum(hot * base_ref[0], axis=0, keepdims=True)
            carry = carry + jnp.sum(hot, axis=1, keepdims=True)
            pos_ref[layer, seq:seq + 1, first:first + LANES] = jnp.where(slot < capacity, base + slot, float(drop)).astype(jnp.int32)


def attn_kernel(layer, head_dim, x_ref, mask_ref, bias_ref, gain_ref, wq_ref, wk_ref, wv_ref, wo_ref,
                h1_ref, b_ref, q_s, k_s, v_s, ctx_s):
    pair = pl.program_id(0)
    pairs = pl.num_programs(0)
    n_pairs, num_seqs, _, width = q_s.shape

    @pl.when(pair == 0)
    def _():
        @pl.loop(0, num_seqs)
        def _(seq):
            a = rms(x_ref[seq].astype(F32), gain_ref[layer, 0:1, :]).astype(BF16)
            for w_ref, dst in ((wq_ref, q_s), (wk_ref, k_s), (wv_ref, v_s)):
                rows = jnp.dot(a, w_ref[...], preferred_element_type=F32).astype(BF16)
                for j in range(n_pairs):
                    dst[j, seq] = rows[:, j * width:(j + 1) * width]

    for seq in range(num_seqs):
        q2, k2, v2 = q_s[pair, seq], k_s[pair, seq], v_s[pair, seq]
        lane = lax.broadcasted_iota(jnp.int32, q2.shape, 1)
        mask_row = jnp.where(mask_ref[seq:seq + 1, :] > 0, 0.0, NEG_BIG)
        parts = []
        for half in range(width // head_dim):
            mine = (lane >= half * head_dim) & (lane < (half + 1) * head_dim)
            qh = jnp.where(mine, q2, jnp.zeros_like(q2))
            s = lax.dot_general(qh, k2, (((1,), (1,)), ((), ())), preferred_element_type=F32)
            s = s + bias_ref[half] + mask_row
            p = jnp.exp(s - jnp.max(s, axis=-1, keepdims=True))
            p = (p * (1.0 / jnp.sum(p, axis=-1, keepdims=True))).astype(BF16)
            o = jnp.dot(p, v2, preferred_element_type=F32)
            parts.append(jnp.where(mine, o, 0.0))
        ctx_s[seq, :, pl.ds(pl.multiple_of(pair * width, width), width)] = sum(parts).astype(BF16)

    @pl.when(pair == pairs - 1)
    def _():
        @pl.loop(0, num_seqs)
        def _(seq):
            o = jnp.dot(ctx_s[seq], wo_ref[...], preferred_element_type=F32)
            h1 = (x_ref[seq].astype(F32) + o).astype(BF16)
            h1_ref[seq] = h1
            b_ref[seq] = rms(h1.astype(F32), gain_ref[layer, 1:2, :]).astype(BF16)


def attention(layer, x, mask, rel_bias, gains, wq, wk, wv, wo):
    num_seqs, seq_len, model_dim = x.shape
    num_heads = rel_bias.shape[0]
    inner = wq.shape[2]
    head_dim = inner // num_heads
    per = LANES // head_dim
    pairs = num_heads // per
    full = lambda *shape: pl.BlockSpec(shape, lambda p: (0,) * len(shape))
    of_layer = lambda *shape: pl.BlockSpec((None,) + shape, lambda p: (layer,) + (0,) * len(shape))
    flops = 2 * num_seqs * seq_len * (4 * model_dim * inner + 2 * seq_len * inner)
    return pl.pallas_call(
        functools.partial(attn_kernel, layer, head_dim),
        grid=(pairs,),
        in_specs=[full(num_seqs, seq_len, model_dim), full(num_seqs, seq_len),
                  pl.BlockSpec((per, seq_len, seq_len), lambda p: (p, 0, 0)), full(*gains.shape),
                  of_layer(model_dim, inner), of_layer(model_dim, inner), of_layer(model_dim, inner),
                  of_layer(inner, model_dim)],
        out_specs=[full(num_seqs, seq_len, model_dim), full(num_seqs, seq_len, model_dim)],
        out_shape=[jax.ShapeDtypeStruct(x.shape, BF16), jax.ShapeDtypeStruct(x.shape, BF16)],
        scratch_shapes=[pltpu.VMEM((pairs, num_seqs, seq_len, LANES), BF16)] * 3
        + [pltpu.VMEM((num_seqs, seq_len, inner), BF16)],
        compiler_params=pltpu.CompilerParams(dimension_semantics=("arbitrary",), vmem_limit_bytes=60 << 20),
        cost_estimate=pl.CostEstimate(flops=flops, bytes_accessed=32 << 20, transcendentals=num_seqs * num_heads * seq_len * seq_len),
        name="attn",
    )(x, mask, rel_bias, gains, wq, wk, wv, wo)


def moe_kernel(layer, axis, pos_ref, e_ref, gain_ref, wr_ref, h1_ref, b_ref, w_in_ref, w_out_ref, out_ref,
               packed, recv, ret, w_in_buf, w_out_buf, acc, u_acc, pos_col, gate_col, out_send, out_recv, back_send, back_recv, w_sem):
    mine, peers, capacity, dim = packed.shape
    num_seqs, seq_len, _ = b_ref.shape
    ff = w_in_buf.shape[2]
    rows = peers * capacity
    me = lax.axis_index(axis)
    other = lambda shift: lax.rem(me + shift, peers)

    def weights(k):
        slot = lax.rem(k, 2)
        return (pltpu.make_async_copy(w_in_ref.at[layer, k], w_in_buf.at[slot], w_sem.at[0, slot]),
                pltpu.make_async_copy(w_out_ref.at[layer, k], w_out_buf.at[slot], w_sem.at[1, slot]))

    def there(k, peer, slot):
        return pltpu.make_async_remote_copy(
            src_ref=packed.at[k, peer], dst_ref=recv.at[k, slot], send_sem=out_send.at[k, peer],
            recv_sem=out_recv.at[k, slot], device_id={axis: peer}, device_id_type=pl.DeviceIdType.MESH)

    def back(k, peer, slot):
        return pltpu.make_async_remote_copy(
            src_ref=recv.at[k, peer], dst_ref=ret.at[k, slot], send_sem=back_send.at[k, peer],
            recv_sem=back_recv.at[k, slot], device_id={axis: peer}, device_id_type=pl.DeviceIdType.MESH)

    def each_peer(fn):
        @pl.loop(1, peers)
        def _(shift):
            fn(other(shift))

    for k in range(min(2, mine)):
        for copy in weights(k):
            copy.start()

    barrier = pltpu.get_barrier_semaphore()
    each_peer(lambda peer: pl.semaphore_signal(barrier, inc=1, device_id={axis: peer}, device_id_type=pl.DeviceIdType.MESH))
    pl.semaphore_wait(barrier, peers - 1)

    half = peers // 2
    @pl.loop(0, mine)
    def _(k):
        @pl.loop(0, 2)
        def _(part):
            first = k * rows + part * (half * capacity)
            want = lax.broadcasted_iota(jnp.int32, (half * capacity, seq_len), 0) + first
            total = None
            for s in range(num_seqs):
                hot = (want == pos_ref[layer, s:s + 1, :]).astype(F32).astype(BF16)
                term = jnp.dot(hot, b_ref[s], preferred_element_type=F32)
                total = term if total is None else total + term
            packed[k, pl.ds(part * half, half)] = total.astype(BF16).reshape(half, capacity, dim)
        each_peer(lambda peer: there(k, peer, me).start())
        recv[k, me] = packed[k, me]

    u_acc[...] = jnp.zeros_like(u_acc)
    column = lambda row: jnp.broadcast_to(row, (LANES, row.shape[1])).T[:, :1]
    for s in range(num_seqs):
        @pl.loop(0, seq_len // 256)
        def _(part):
            tok = pl.ds(pl.multiple_of(part * 256, 256), 256)
            pos_col[s, tok, :] = column(pos_ref[layer, s:s + 1, tok].astype(F32)).astype(jnp.int32)
            r = rms(h1_ref[s, tok, :].astype(F32), gain_ref[layer, 1:2, :])
            logits = lax.dot_general(wr_ref[layer], r, (((1,), (1,)), ((), ())),
                                     precision=lax.Precision.HIGHEST, preferred_element_type=F32)
            ex = jnp.exp(logits - jnp.max(logits, axis=0, keepdims=True))
            chosen = lax.broadcasted_iota(jnp.int32, ex.shape, 0) == e_ref[layer, s:s + 1, tok]
            gate = jnp.sum(jnp.where(chosen, ex, 0.0), axis=0, keepdims=True) / jnp.sum(ex, axis=0, keepdims=True)
            gate_col[s, tok, :] = column(gate)

    @pl.loop(0, mine)
    def _(k):
        slot = lax.rem(k, 2)
        for copy in weights(k):
            copy.wait()
        each_peer(lambda peer: there(k, peer, peer).wait_recv())
        acc[...] = jnp.zeros_like(acc)

        @pl.loop(0, ff // dim)
        def _(part):
            cols = pl.ds(pl.multiple_of(part * dim, dim), dim)
            act = jnp.dot(recv[k].reshape(rows, dim), w_in_buf[slot, :, cols], preferred_element_type=F32)
            act = jnp.maximum(act, 0.0).astype(BF16)
            acc[...] += jnp.dot(act, w_out_buf[slot, cols, :], preferred_element_type=F32)

        recv[k] = acc[...].astype(BF16).reshape(peers, capacity, dim)
        each_peer(lambda peer: back(k, peer, me).start())
        ret[k, me] = recv[k, me]

        @pl.when(k + 2 < mine)
        def _():
            for copy in weights(k + 2):
                copy.start()

    def gather_back(k, last):
        each_peer(lambda peer: back(k, peer, peer).wait_recv())
        for s in range(num_seqs):
            @pl.loop(0, seq_len // 256)
            def _(part):
                tok = pl.ds(pl.multiple_of(part * 256, 256), 256)
                want = lax.broadcasted_iota(jnp.int32, (256, rows), 1) + k * rows
                hot = (want == pos_col[s, tok, :]).astype(F32).astype(BF16)
                u = jnp.dot(hot, ret[k].reshape(rows, dim), preferred_element_type=F32) + u_acc[s, tok, :].astype(F32)
                if last:
                    out_ref[s, tok, :] = (h1_ref[s, tok, :].astype(F32) + gate_col[s, tok, :] * u).astype(BF16)
                else:
                    u_acc[s, tok, :] = u.astype(BF16)

    @pl.loop(0, mine - 1)
    def _(k):
        gather_back(k, False)

    gather_back(mine - 1, True)

    @pl.loop(0, mine)
    def _(k):
        each_peer(lambda peer: there(k, peer, me).wait_send())
        each_peer(lambda peer: back(k, peer, me).wait_send())


def moe(layer, axis, peers, capacity, pos, expert_idx, gains, w_router_t, h1, b, w_in, w_out):
    num_seqs, seq_len, dim = h1.shape
    mine, _, ff = w_in.shape[1:]
    rows = peers * capacity
    near = pl.BlockSpec(memory_space=pltpu.VMEM)
    hbm = pl.BlockSpec(memory_space=pl.ANY)
    buffer = pltpu.VMEM((mine, peers, capacity, dim), BF16)
    sems = pltpu.SemaphoreType.DMA((mine, peers))
    return pl.pallas_call(
        functools.partial(moe_kernel, layer, axis),
        in_specs=[near] * 6 + [hbm, hbm],
        out_specs=near,
        out_shape=jax.ShapeDtypeStruct(h1.shape, BF16),
        scratch_shapes=[buffer, buffer, buffer, pltpu.VMEM((2, dim, ff), BF16), pltpu.VMEM((2, ff, dim), BF16),
                        pltpu.VMEM((rows, dim), F32), pltpu.VMEM((num_seqs, seq_len, dim), BF16),
                        pltpu.VMEM((num_seqs, seq_len, 1), jnp.int32), pltpu.VMEM((num_seqs, seq_len, 1), F32),
                        sems, sems, sems, sems, pltpu.SemaphoreType.DMA((2, 2))],
        compiler_params=pltpu.CompilerParams(collective_id=layer, has_side_effects=True, vmem_limit_bytes=67043328),
        cost_estimate=pl.CostEstimate(flops=4 * mine * rows * dim * ff, bytes_accessed=48 << 20, transcendentals=0),
        name="moe",
    )(pos, expert_idx, gains, w_router_t, h1, b, w_in, w_out)


def solution(mesh):
    token_spec = P(('dp', 'ep'))
    peers = mesh.shape['ep']

    def per_device(x_in, pad_mask, rel_bias, expert_idx, norm_scale, w_query, w_key, w_value, w_attn_out, w_router, w_in, w_out):
        num_seqs, seq_len, model_dim = x_in.shape
        tok_count = num_seqs * seq_len
        layers = w_router.shape[0]
        num_experts = w_router.shape[2]
        mine = num_experts // peers
        capacity = (CAP_FACTOR * tok_count + num_experts - 1) // num_experts
        slots = num_experts * capacity
        expert_ids = jnp.arange(num_experts, dtype=jnp.int32)
        base = ((expert_ids % mine) * (peers * capacity) + (expert_ids // mine) * capacity).astype(F32)
        pos = pl.pallas_call(
            functools.partial(slots_kernel, capacity, slots),
            out_shape=jax.ShapeDtypeStruct(expert_idx.shape, jnp.int32),
            name="slots",
        )(expert_idx, base.reshape(1, num_experts, 1))
        w_router_t = jnp.swapaxes(w_router, 1, 2)
        hidden = x_in
        for layer in range(layers):
            h1, b = attention(layer, hidden, pad_mask, rel_bias, norm_scale, w_query, w_key, w_value, w_attn_out)
            hidden = moe(layer, 'ep', peers, capacity, pos, expert_idx, norm_scale, w_router_t, h1, b, w_in, w_out)
        return hidden

    return jax.shard_map(per_device, mesh=mesh, in_specs=(token_spec, token_spec, P(), P(None, ('dp', 'ep')), P(), P(), P(), P(), P(), P(), P(None, 'ep'), P(None, 'ep')), out_specs=token_spec, check_vma=False)
```

```python
import functools

import jax
import jax.numpy as jnp
from jax import lax
from jax.experimental import pallas as pl
from jax.experimental.pallas import tpu as pltpu
from jax.sharding import PartitionSpec as P

NORM_EPS = 1e-6
NEG_BIG = -1e9
CAP_FACTOR = 2
LANES = 128
F32 = jnp.float32
BF16 = jnp.bfloat16


def rms(hid32, gain):
    return hid32 * lax.rsqrt(jnp.mean(hid32 * hid32, axis=-1, keepdims=True) + NORM_EPS) * gain


def slots_kernel(capacity, mine, num_experts, e_ref, pos_ref):
    num_seqs, layers, seq_len = e_ref.shape
    drop = num_experts * capacity
    row = lax.broadcasted_iota(jnp.int32, (LANES, LANES), 0)
    col = lax.broadcasted_iota(jnp.int32, (LANES, LANES), 1)
    upper = (row <= col).astype(F32).astype(BF16)
    experts = lax.broadcasted_iota(jnp.int32, (num_experts, LANES), 0)
    number = lax.broadcasted_iota(jnp.int32, (num_experts, 1), 0).astype(F32)
    owner = jnp.floor((number + 0.5) * (1.0 / mine))
    base_of = (number - owner * mine) * (num_experts // mine * capacity) + owner * capacity
    for layer in range(layers):
        carry = jnp.zeros((num_experts, 1), F32)
        for blk in range(num_seqs * seq_len // LANES):
            seq, first = divmod(blk * LANES, seq_len)
            hit = experts == e_ref[seq, layer:layer + 1, first:first + LANES]
            hot = hit.astype(F32)
            cum = jnp.dot(hot.astype(BF16), upper, preferred_element_type=F32) + (carry - 1.0)
            slot = jnp.sum(hot * cum, axis=0, keepdims=True)
            base = jnp.sum(hot * base_of, axis=0, keepdims=True)
            carry = carry + jnp.sum(hot, axis=1, keepdims=True)
            pos_ref[seq, layer:layer + 1, first:first + LANES] = jnp.where(slot < capacity, base + slot, float(drop)).astype(jnp.int32)


def attn_kernel(layer, head_dim, x_hbm, mask_ref, bias_ref, gain_ref, wq_hbm, wk_hbm, wv_hbm, wo_hbm,
                h1_hbm, b_hbm, x_ref, h1_ref, b_ref, w_ref, q_s, k_s, v_s, ctx_s, x_sem, w_sem, out_sem):
    pair = pl.program_id(0)
    pairs = pl.num_programs(0)
    n_pairs, num_seqs, _, width = q_s.shape
    x_in = lambda seq: pltpu.make_async_copy(x_hbm.at[seq], x_ref.at[seq], x_sem.at[seq])
    weight = lambda i: pltpu.make_async_copy((wq_hbm, wk_hbm, wv_hbm, wo_hbm)[i].at[layer], w_ref.at[i], w_sem.at[i])
    h1_out = lambda seq: pltpu.make_async_copy(h1_ref.at[seq], h1_hbm.at[seq], out_sem.at[0, seq])
    b_out = lambda seq: pltpu.make_async_copy(b_ref.at[seq], b_hbm.at[seq], out_sem.at[1, seq])

    @pl.when(pair == 0)
    def _():
        x_in(0).start()
        for i in range(3):
            weight(i).start()
        for seq in range(1, num_seqs):
            x_in(seq).start()
        weight(3).start()

        @pl.loop(0, num_seqs)
        def _(seq):
            x_in(seq).wait()
            a = rms(x_ref[seq].astype(F32), gain_ref[layer, 0:1, :]).astype(BF16)

            @pl.when(seq == 0)
            def _():
                for i in range(3):
                    weight(i).wait()

            for i, dst in enumerate((q_s, k_s, v_s)):
                rows = jnp.dot(a, w_ref[i], preferred_element_type=F32).astype(BF16)
                for j in range(n_pairs):
                    dst[j, seq] = rows[:, j * width:(j + 1) * width]

    for seq in range(num_seqs):
        q2, k2, v2 = q_s[pair, seq], k_s[pair, seq], v_s[pair, seq]
        lane = lax.broadcasted_iota(jnp.int32, q2.shape, 1)
        mask_row = jnp.where(mask_ref[seq:seq + 1, :] > 0, 0.0, NEG_BIG)
        parts = []
        for half in range(width // head_dim):
            mine = (lane >= half * head_dim) & (lane < (half + 1) * head_dim)
            qh = jnp.where(mine, q2, jnp.zeros_like(q2))
            s = lax.dot_general(qh, k2, (((1,), (1,)), ((), ())), preferred_element_type=F32)
            s = s + bias_ref[half] + mask_row
            p = jnp.exp(s - jnp.max(s, axis=-1, keepdims=True))
            p = (p * (1.0 / jnp.sum(p, axis=-1, keepdims=True))).astype(BF16)
            o = jnp.dot(p, v2, preferred_element_type=F32)
            parts.append(jnp.where(mine, o, 0.0))
        ctx_s[seq, :, pl.ds(pl.multiple_of(pair * width, width), width)] = sum(parts).astype(BF16)

    @pl.when(pair == pairs - 1)
    def _():
        weight(3).wait()

        @pl.loop(0, num_seqs)
        def _(seq):
            o = jnp.dot(ctx_s[seq], w_ref[3], preferred_element_type=F32)
            h1 = (x_ref[seq].astype(F32) + o).astype(BF16)
            h1_ref[seq] = h1
            b_ref[seq] = rms(h1.astype(F32), gain_ref[layer, 1:2, :]).astype(BF16)
            h1_out(seq).start()
            b_out(seq).start()

        for seq in range(num_seqs):
            h1_out(seq).wait()
            b_out(seq).wait()


def attention(layer, x, mask, rel_bias, gains, wq, wk, wv, wo):
    num_seqs, seq_len, model_dim = x.shape
    num_heads = rel_bias.shape[0]
    inner = wq.shape[2]
    head_dim = inner // num_heads
    per = LANES // head_dim
    pairs = num_heads // per
    full = lambda *shape: pl.BlockSpec(shape, lambda p: (0,) * len(shape))
    hbm = pl.BlockSpec(memory_space=pl.ANY)
    flops = 2 * num_seqs * seq_len * (4 * model_dim * inner + 2 * seq_len * inner)
    return pl.pallas_call(
        functools.partial(attn_kernel, layer, head_dim),
        grid=(pairs,),
        in_specs=[hbm, full(num_seqs, seq_len), pl.BlockSpec((per, seq_len, seq_len), lambda p: (p, 0, 0)),
                  full(*gains.shape), hbm, hbm, hbm, hbm],
        out_specs=[hbm, hbm],
        out_shape=[jax.ShapeDtypeStruct(x.shape, BF16), jax.ShapeDtypeStruct(x.shape, BF16)],
        scratch_shapes=[pltpu.VMEM(x.shape, BF16)] * 3 + [pltpu.VMEM((4, model_dim, inner), BF16)]
        + [pltpu.VMEM((pairs, num_seqs, seq_len, LANES), BF16)] * 3 + [pltpu.VMEM((num_seqs, seq_len, inner), BF16)]
        + [pltpu.SemaphoreType.DMA((num_seqs,)), pltpu.SemaphoreType.DMA((4,)), pltpu.SemaphoreType.DMA((2, num_seqs))],
        compiler_params=pltpu.CompilerParams(dimension_semantics=("arbitrary",), vmem_limit_bytes=60 << 20),
        cost_estimate=pl.CostEstimate(flops=flops, bytes_accessed=32 << 20, transcendentals=num_seqs * num_heads * seq_len * seq_len),
        name="attn",
    )(x, mask, rel_bias, gains, wq, wk, wv, wo)


def moe_kernel(layer, axis, pos_ref, e_ref, gain_ref, wr_ref, b_ref, h1_hbm, w_in_ref, w_out_ref, out_ref,
               h1_ref, packed, recv, ret, w_in_buf, w_out_buf, acc, u_acc, pos_col, gate_col, out_send, out_recv, back_send, back_recv, w_sem, h1_sem):
    mine, peers, capacity, dim = packed.shape
    num_seqs, seq_len, _ = b_ref.shape
    ff = w_in_buf.shape[2]
    rows = peers * capacity
    me = lax.axis_index(axis)
    other = lambda shift: lax.rem(me + shift, peers)

    def weights(k):
        slot = lax.rem(k, 2)
        return (pltpu.make_async_copy(w_in_ref.at[layer, k], w_in_buf.at[slot], w_sem.at[0, slot]),
                pltpu.make_async_copy(w_out_ref.at[layer, k], w_out_buf.at[slot], w_sem.at[1, slot]))

    def there(k, peer, slot):
        return pltpu.make_async_remote_copy(
            src_ref=packed.at[k, peer], dst_ref=recv.at[k, slot], send_sem=out_send.at[k, peer],
            recv_sem=out_recv.at[k, slot], device_id={axis: peer}, device_id_type=pl.DeviceIdType.MESH)

    def back(k, peer, slot):
        return pltpu.make_async_remote_copy(
            src_ref=recv.at[k, peer], dst_ref=ret.at[k, slot], send_sem=back_send.at[k, peer],
            recv_sem=back_recv.at[k, slot], device_id={axis: peer}, device_id_type=pl.DeviceIdType.MESH)

    def each_peer(fn):
        @pl.loop(1, peers)
        def _(shift):
            fn(other(shift))

    h1_in = pltpu.make_async_copy(h1_hbm, h1_ref, h1_sem)
    h1_in.start()
    for k in range(min(2, mine)):
        for copy in weights(k):
            copy.start()

    barrier = pltpu.get_barrier_semaphore()
    each_peer(lambda peer: pl.semaphore_signal(barrier, inc=1, device_id={axis: peer}, device_id_type=pl.DeviceIdType.MESH))
    pl.semaphore_wait(barrier, peers - 1)

    half = peers // 2
    @pl.loop(0, mine)
    def _(k):
        @pl.loop(0, 2)
        def _(part):
            first = k * rows + part * (half * capacity)
            want = lax.broadcasted_iota(jnp.int32, (half * capacity, seq_len), 0) + first
            total = None
            for s in range(num_seqs):
                hot = (want == pos_ref[s, layer:layer + 1, :]).astype(F32).astype(BF16)
                term = jnp.dot(hot, b_ref[s], preferred_element_type=F32)
                total = term if total is None else total + term
            packed[k, pl.ds(part * half, half)] = total.astype(BF16).reshape(half, capacity, dim)

            @pl.loop(0, half)
            def _(i):
                peer = part * half + lax.rem(me + i, half)

                @pl.when(peer != me)
                def _():
                    there(k, peer, me).start()

        recv[k, me] = packed[k, me]

    u_acc[...] = jnp.zeros_like(u_acc)
    h1_in.wait()
    column = lambda row: jnp.broadcast_to(row, (LANES, row.shape[1])).T[:, :1]
    for s in range(num_seqs):
        @pl.loop(0, seq_len // 256)
        def _(part):
            tok = pl.ds(pl.multiple_of(part * 256, 256), 256)
            pos_col[s, tok, :] = column(pos_ref[s, layer:layer + 1, tok].astype(F32)).astype(jnp.int32)
            r = rms(h1_ref[s, tok, :].astype(F32), gain_ref[layer, 1:2, :])
            logits = lax.dot_general(wr_ref[layer], r, (((1,), (1,)), ((), ())),
                                     precision=lax.Precision.HIGHEST, preferred_element_type=F32)
            ex = jnp.exp(logits - jnp.max(logits, axis=0, keepdims=True))
            chosen = lax.broadcasted_iota(jnp.int32, ex.shape, 0) == e_ref[s, layer:layer + 1, tok]
            gate = jnp.sum(jnp.where(chosen, ex, 0.0), axis=0, keepdims=True) / jnp.sum(ex, axis=0, keepdims=True)
            gate_col[s, tok, :] = column(gate)

    @pl.loop(0, mine)
    def _(k):
        slot = lax.rem(k, 2)
        for copy in weights(k):
            copy.wait()
        each_peer(lambda peer: there(k, peer, peer).wait_recv())
        acc[...] = jnp.zeros_like(acc)

        @pl.loop(0, ff // dim)
        def _(part):
            cols = pl.ds(pl.multiple_of(part * dim, dim), dim)
            act = jnp.dot(recv[k].reshape(rows, dim), w_in_buf[slot, :, cols], preferred_element_type=F32)
            act = jnp.maximum(act, 0.0).astype(BF16)
            acc[...] += jnp.dot(act, w_out_buf[slot, cols, :], preferred_element_type=F32)

        recv[k] = acc[...].astype(BF16).reshape(peers, capacity, dim)
        each_peer(lambda peer: back(k, peer, me).start())
        ret[k, me] = recv[k, me]

        @pl.when(k + 2 < mine)
        def _():
            for copy in weights(k + 2):
                copy.start()

    def gather_back(k, first, count, last):
        @pl.loop(first, first + count)
        def _(peer):
            @pl.when(peer != me)
            def _():
                back(k, peer, peer).wait_recv()

        for s in range(num_seqs):
            @pl.loop(0, seq_len // 256)
            def _(part):
                tok = pl.ds(pl.multiple_of(part * 256, 256), 256)
                want = lax.broadcasted_iota(jnp.int32, (256, count * capacity), 1) + (k * rows + first * capacity)
                hot = (want == pos_col[s, tok, :]).astype(F32).astype(BF16)
                u = jnp.dot(hot, ret[k, pl.ds(first, count)].reshape(count * capacity, dim), preferred_element_type=F32)
                u = u + u_acc[s, tok, :].astype(F32)
                if last:
                    out_ref[s, tok, :] = (h1_ref[s, tok, :].astype(F32) + gate_col[s, tok, :] * u).astype(BF16)
                else:
                    u_acc[s, tok, :] = u.astype(BF16)

    @pl.loop(0, mine - 1)
    def _(k):
        gather_back(k, 0, peers, False)

    gather_back(mine - 1, 0, half, False)
    gather_back(mine - 1, half, peers - half, True)

    @pl.loop(0, mine)
    def _(k):
        each_peer(lambda peer: there(k, peer, me).wait_send())
        each_peer(lambda peer: back(k, peer, me).wait_send())


def moe(layer, axis, peers, capacity, pos, ids, gains, w_router_t, h1, b, w_in, w_out):
    num_seqs, seq_len, dim = h1.shape
    mine, _, ff = w_in.shape[1:]
    rows = peers * capacity
    near = pl.BlockSpec(memory_space=pltpu.VMEM)
    hbm = pl.BlockSpec(memory_space=pl.ANY)
    buffer = pltpu.VMEM((mine, peers, capacity, dim), BF16)
    sems = pltpu.SemaphoreType.DMA((mine, peers))
    return pl.pallas_call(
        functools.partial(moe_kernel, layer, axis),
        in_specs=[near] * 5 + [hbm] * 3,
        out_specs=near,
        out_shape=jax.ShapeDtypeStruct(h1.shape, BF16),
        scratch_shapes=[pltpu.VMEM(h1.shape, BF16), buffer, buffer, buffer, pltpu.VMEM((2, dim, ff), BF16), pltpu.VMEM((2, ff, dim), BF16),
                        pltpu.VMEM((rows, dim), F32), pltpu.VMEM((num_seqs, seq_len, dim), BF16),
                        pltpu.VMEM((num_seqs, seq_len, 1), jnp.int32), pltpu.VMEM((num_seqs, seq_len, 1), F32),
                        sems, sems, sems, sems, pltpu.SemaphoreType.DMA((2, 2)), pltpu.SemaphoreType.DMA(())],
        compiler_params=pltpu.CompilerParams(collective_id=layer, has_side_effects=True, vmem_limit_bytes=67043328),
        cost_estimate=pl.CostEstimate(flops=4 * mine * rows * dim * ff, bytes_accessed=48 << 20, transcendentals=0),
        name="moe",
    )(pos, ids, gains, w_router_t, b, h1, w_in, w_out)


def solution(mesh):
    token_spec = P(('dp', 'ep'))
    peers = mesh.shape['ep']

    def per_device(x_in, pad_mask, rel_bias, expert_idx, norm_scale, w_query, w_key, w_value, w_attn_out, w_router, w_in, w_out):
        num_seqs, seq_len, model_dim = x_in.shape
        tok_count = num_seqs * seq_len
        layers = w_router.shape[0]
        num_experts = w_router.shape[2]
        mine = num_experts // peers
        capacity = (CAP_FACTOR * tok_count + num_experts - 1) // num_experts
        ids = jnp.swapaxes(expert_idx, 0, 1)
        pos = pl.pallas_call(
            functools.partial(slots_kernel, capacity, mine, num_experts),
            out_shape=jax.ShapeDtypeStruct(ids.shape, jnp.int32),
            name="slots",
        )(ids)
        w_router_t = jnp.swapaxes(w_router, 1, 2)
        hidden = x_in
        for layer in range(layers):
            h1, b = attention(layer, hidden, pad_mask, rel_bias, norm_scale, w_query, w_key, w_value, w_attn_out)
            hidden = moe(layer, 'ep', peers, capacity, pos, ids, norm_scale, w_router_t, h1, b, w_in, w_out)
        return hidden

    return jax.shard_map(per_device, mesh=mesh, in_specs=(token_spec, token_spec, P(), P(None, ('dp', 'ep')), P(), P(), P(), P(), P(), P(), P(None, 'ep'), P(None, 'ep')), out_specs=token_spec, check_vma=False)
```

```python
import functools

import jax
import jax.numpy as jnp
from jax import lax
from jax.experimental import pallas as pl
from jax.experimental.pallas import tpu as pltpu
from jax.sharding import PartitionSpec as P

NORM_EPS = 1e-6
NEG_BIG = -1e9
CAP_FACTOR = 2
LANES = 128
F32 = jnp.float32
BF16 = jnp.bfloat16


def rms(hid32, gain):
    return hid32 * lax.rsqrt(jnp.mean(hid32 * hid32, axis=-1, keepdims=True) + NORM_EPS) * gain


def slots_kernel(capacity, mine, num_experts, e_ref, pos_ref):
    num_seqs, layers, seq_len = e_ref.shape
    drop = num_experts * capacity
    row = lax.broadcasted_iota(jnp.int32, (LANES, LANES), 0)
    col = lax.broadcasted_iota(jnp.int32, (LANES, LANES), 1)
    upper = (row <= col).astype(F32).astype(BF16)
    experts = lax.broadcasted_iota(jnp.int32, (num_experts, LANES), 0)
    number = lax.broadcasted_iota(jnp.int32, (num_experts, 1), 0).astype(F32)
    owner = jnp.floor((number + 0.5) * (1.0 / mine))
    base_of = (number - owner * mine) * (num_experts // mine * capacity) + owner * capacity
    for layer in range(layers):
        carry = jnp.zeros((num_experts, 1), F32)
        for blk in range(num_seqs * seq_len // LANES):
            seq, first = divmod(blk * LANES, seq_len)
            hit = experts == e_ref[seq, layer:layer + 1, first:first + LANES]
            hot = hit.astype(F32)
            cum = jnp.dot(hot.astype(BF16), upper, preferred_element_type=F32) + (carry - 1.0)
            slot = jnp.sum(hot * cum, axis=0, keepdims=True)
            base = jnp.sum(hot * base_of, axis=0, keepdims=True)
            carry = carry + jnp.sum(hot, axis=1, keepdims=True)
            pos_ref[seq, layer:layer + 1, first:first + LANES] = jnp.where(slot < capacity, base + slot, float(drop)).astype(jnp.int32)


def attn_kernel(layer, head_dim, x_hbm, mask_ref, bias_ref, gain_ref, wq_hbm, wk_hbm, wv_hbm, wo_hbm,
                h1_hbm, b_hbm, x_ref, h1_ref, b_ref, w_ref, q_s, k_s, v_s, ctx_s, x_sem, w_sem, out_sem):
    pair = pl.program_id(0)
    pairs = pl.num_programs(0)
    n_pairs, num_seqs, _, width = q_s.shape
    x_in = lambda seq: pltpu.make_async_copy(x_hbm.at[seq], x_ref.at[seq], x_sem.at[seq])
    weight = lambda i: pltpu.make_async_copy((wq_hbm, wk_hbm, wv_hbm, wo_hbm)[i].at[layer], w_ref.at[i], w_sem.at[i])
    h1_out = lambda seq: pltpu.make_async_copy(h1_ref.at[seq], h1_hbm.at[seq], out_sem.at[0, seq])
    b_out = lambda seq: pltpu.make_async_copy(b_ref.at[seq], b_hbm.at[seq], out_sem.at[1, seq])

    @pl.when(pair == 0)
    def _():
        x_in(0).start()
        for i in range(3):
            weight(i).start()
        for seq in range(1, num_seqs):
            x_in(seq).start()
        weight(3).start()

        @pl.loop(0, num_seqs)
        def _(seq):
            x_in(seq).wait()
            a = rms(x_ref[seq].astype(F32), gain_ref[layer, 0:1, :]).astype(BF16)

            @pl.when(seq == 0)
            def _():
                for i in range(3):
                    weight(i).wait()

            for i, dst in enumerate((q_s, k_s, v_s)):
                rows = jnp.dot(a, w_ref[i], preferred_element_type=F32).astype(BF16)
                for j in range(n_pairs):
                    dst[j, seq] = rows[:, j * width:(j + 1) * width]

    for seq in range(num_seqs):
        q2, k2, v2 = q_s[pair, seq], k_s[pair, seq], v_s[pair, seq]
        lane = lax.broadcasted_iota(jnp.int32, q2.shape, 1)
        mask_row = jnp.where(mask_ref[seq:seq + 1, :] > 0, 0.0, NEG_BIG)
        parts = []
        for half in range(width // head_dim):
            mine = (lane >= half * head_dim) & (lane < (half + 1) * head_dim)
            qh = jnp.where(mine, q2, jnp.zeros_like(q2))
            s = lax.dot_general(qh, k2, (((1,), (1,)), ((), ())), preferred_element_type=F32)
            s = s + bias_ref[half] + mask_row
            p = jnp.exp(s - jnp.max(s, axis=-1, keepdims=True))
            p = (p * (1.0 / jnp.sum(p, axis=-1, keepdims=True))).astype(BF16)
            o = jnp.dot(p, v2, preferred_element_type=F32)
            parts.append(jnp.where(mine, o, 0.0))
        ctx_s[seq, :, pl.ds(pl.multiple_of(pair * width, width), width)] = sum(parts).astype(BF16)

    @pl.when(pair == pairs - 1)
    def _():
        weight(3).wait()

        @pl.loop(0, num_seqs)
        def _(seq):
            o = jnp.dot(ctx_s[seq], w_ref[3], preferred_element_type=F32)
            h1 = (x_ref[seq].astype(F32) + o).astype(BF16)
            h1_ref[seq] = h1
            b_ref[seq] = rms(h1.astype(F32), gain_ref[layer, 1:2, :]).astype(BF16)
            h1_out(seq).start()
            b_out(seq).start()

        for seq in range(num_seqs):
            h1_out(seq).wait()
            b_out(seq).wait()


def attention(layer, x, mask, rel_bias, gains, wq, wk, wv, wo):
    num_seqs, seq_len, model_dim = x.shape
    num_heads = rel_bias.shape[0]
    inner = wq.shape[2]
    head_dim = inner // num_heads
    per = LANES // head_dim
    pairs = num_heads // per
    full = lambda *shape: pl.BlockSpec(shape, lambda p: (0,) * len(shape))
    hbm = pl.BlockSpec(memory_space=pl.ANY)
    flops = 2 * num_seqs * seq_len * (4 * model_dim * inner + 2 * seq_len * inner)
    return pl.pallas_call(
        functools.partial(attn_kernel, layer, head_dim),
        grid=(pairs,),
        in_specs=[hbm, full(num_seqs, seq_len), pl.BlockSpec((per, seq_len, seq_len), lambda p: (p, 0, 0)),
                  full(*gains.shape), hbm, hbm, hbm, hbm],
        out_specs=[hbm, hbm],
        out_shape=[jax.ShapeDtypeStruct(x.shape, BF16), jax.ShapeDtypeStruct(x.shape, BF16)],
        scratch_shapes=[pltpu.VMEM(x.shape, BF16)] * 3 + [pltpu.VMEM((4, model_dim, inner), BF16)]
        + [pltpu.VMEM((pairs, num_seqs, seq_len, LANES), BF16)] * 3 + [pltpu.VMEM((num_seqs, seq_len, inner), BF16)]
        + [pltpu.SemaphoreType.DMA((num_seqs,)), pltpu.SemaphoreType.DMA((4,)), pltpu.SemaphoreType.DMA((2, num_seqs))],
        compiler_params=pltpu.CompilerParams(dimension_semantics=("arbitrary",), vmem_limit_bytes=60 << 20),
        cost_estimate=pl.CostEstimate(flops=flops, bytes_accessed=32 << 20, transcendentals=num_seqs * num_heads * seq_len * seq_len),
        name="attn",
    )(x, mask, rel_bias, gains, wq, wk, wv, wo)


def moe_kernel(layer, axis, pos_ref, e_ref, gain_ref, wr_ref, b_hbm, h1_hbm, w_in_ref, w_out_ref, out_ref,
               b_ref, h1_ref, packed, recv, ret, w_in_buf, w_out_buf, acc, u_acc, pos_col, gate_col, out_send, out_recv, back_send, back_recv, w_sem, x_sem):
    mine, peers, capacity, dim = packed.shape
    num_seqs, seq_len, _ = b_ref.shape
    ff = w_in_buf.shape[2]
    rows = peers * capacity
    me = lax.axis_index(axis)
    other = lambda shift: lax.rem(me + shift, peers)

    def weights(k):
        slot = lax.rem(k, 2)
        return (pltpu.make_async_copy(w_in_ref.at[layer, k], w_in_buf.at[slot], w_sem.at[0, slot]),
                pltpu.make_async_copy(w_out_ref.at[layer, k], w_out_buf.at[slot], w_sem.at[1, slot]))

    def there(k, peer, slot):
        return pltpu.make_async_remote_copy(
            src_ref=packed.at[k, peer], dst_ref=recv.at[k, slot], send_sem=out_send.at[k, peer],
            recv_sem=out_recv.at[k, slot], device_id={axis: peer}, device_id_type=pl.DeviceIdType.MESH)

    def back(k, peer, slot):
        return pltpu.make_async_remote_copy(
            src_ref=recv.at[k, peer], dst_ref=ret.at[k, slot], send_sem=back_send.at[k, peer],
            recv_sem=back_recv.at[k, slot], device_id={axis: peer}, device_id_type=pl.DeviceIdType.MESH)

    def each_peer(fn):
        @pl.loop(1, peers)
        def _(shift):
            fn(other(shift))

    b_in = pltpu.make_async_copy(b_hbm, b_ref, x_sem.at[0])
    h1_in = pltpu.make_async_copy(h1_hbm, h1_ref, x_sem.at[1])
    b_in.start()
    barrier = pltpu.get_barrier_semaphore()
    each_peer(lambda peer: pl.semaphore_signal(barrier, inc=1, device_id={axis: peer}, device_id_type=pl.DeviceIdType.MESH))
    half = peers // 2

    def pack(k, part):
        first = k * rows + part * (half * capacity)
        want = lax.broadcasted_iota(jnp.int32, (half * capacity, seq_len), 0) + first
        total = None
        for s in range(num_seqs):
            hot = (want == pos_ref[s, layer:layer + 1, :]).astype(F32).astype(BF16)
            term = jnp.dot(hot, b_ref[s], preferred_element_type=F32)
            total = term if total is None else total + term
        packed[k, pl.ds(part * half, half)] = total.astype(BF16).reshape(half, capacity, dim)

    def send(k, part):
        @pl.loop(0, half)
        def _(i):
            peer = part * half + lax.rem(me + i, half)

            @pl.when(peer != me)
            def _():
                there(k, peer, me).start()

    b_in.wait()
    pack(0, 0)
    pl.semaphore_wait(barrier, peers - 1)
    send(0, 0)
    h1_in.start()
    for k in range(min(2, mine)):
        for copy in weights(k):
            copy.start()

    @pl.loop(1, 2 * mine)
    def _(step):
        pack(step // 2, step % 2)
        send(step // 2, step % 2)

    @pl.loop(0, mine)
    def _(k):
        recv[k, me] = packed[k, me]

    u_acc[...] = jnp.zeros_like(u_acc)
    h1_in.wait()
    column = lambda row: jnp.broadcast_to(row, (LANES, row.shape[1])).T[:, :1]
    for s in range(num_seqs):
        @pl.loop(0, seq_len // 256)
        def _(part):
            tok = pl.ds(pl.multiple_of(part * 256, 256), 256)
            pos_col[s, tok, :] = column(pos_ref[s, layer:layer + 1, tok].astype(F32)).astype(jnp.int32)
            r = rms(h1_ref[s, tok, :].astype(F32), gain_ref[layer, 1:2, :])
            logits = lax.dot_general(wr_ref[layer], r, (((1,), (1,)), ((), ())),
                                     precision=lax.Precision.HIGHEST, preferred_element_type=F32)
            ex = jnp.exp(logits - jnp.max(logits, axis=0, keepdims=True))
            chosen = lax.broadcasted_iota(jnp.int32, ex.shape, 0) == e_ref[s, layer:layer + 1, tok]
            gate = jnp.sum(jnp.where(chosen, ex, 0.0), axis=0, keepdims=True) / jnp.sum(ex, axis=0, keepdims=True)
            gate_col[s, tok, :] = column(gate)

    @pl.loop(0, mine)
    def _(k):
        slot = lax.rem(k, 2)
        for copy in weights(k):
            copy.wait()
        each_peer(lambda peer: there(k, peer, peer).wait_recv())
        acc[...] = jnp.zeros_like(acc)

        @pl.loop(0, ff // dim)
        def _(part):
            cols = pl.ds(pl.multiple_of(part * dim, dim), dim)
            act = jnp.dot(recv[k].reshape(rows, dim), w_in_buf[slot, :, cols], preferred_element_type=F32)
            act = jnp.maximum(act, 0.0).astype(BF16)
            acc[...] += jnp.dot(act, w_out_buf[slot, cols, :], preferred_element_type=F32)

        recv[k] = acc[...].astype(BF16).reshape(peers, capacity, dim)
        each_peer(lambda peer: back(k, peer, me).start())
        ret[k, me] = recv[k, me]

        @pl.when(k + 2 < mine)
        def _():
            for copy in weights(k + 2):
                copy.start()

    def gather_back(k, first, count, last):
        @pl.loop(first, first + count)
        def _(peer):
            @pl.when(peer != me)
            def _():
                back(k, peer, peer).wait_recv()

        for s in range(num_seqs):
            @pl.loop(0, seq_len // 256)
            def _(part):
                tok = pl.ds(pl.multiple_of(part * 256, 256), 256)
                want = lax.broadcasted_iota(jnp.int32, (256, count * capacity), 1) + (k * rows + first * capacity)
                hot = (want == pos_col[s, tok, :]).astype(F32).astype(BF16)
                u = jnp.dot(hot, ret[k, pl.ds(first, count)].reshape(count * capacity, dim), preferred_element_type=F32)
                u = u + u_acc[s, tok, :].astype(F32)
                if last:
                    out_ref[s, tok, :] = (h1_ref[s, tok, :].astype(F32) + gate_col[s, tok, :] * u).astype(BF16)
                else:
                    u_acc[s, tok, :] = u.astype(BF16)

    @pl.loop(0, mine - 1)
    def _(k):
        gather_back(k, 0, peers, False)

    gather_back(mine - 1, 0, half, False)
    gather_back(mine - 1, half, peers - half, True)

    @pl.loop(0, mine)
    def _(k):
        each_peer(lambda peer: there(k, peer, me).wait_send())
        each_peer(lambda peer: back(k, peer, me).wait_send())


def moe(layer, axis, peers, capacity, pos, ids, gains, w_router_t, h1, b, w_in, w_out):
    num_seqs, seq_len, dim = h1.shape
    mine, _, ff = w_in.shape[1:]
    rows = peers * capacity
    near = pl.BlockSpec(memory_space=pltpu.VMEM)
    hbm = pl.BlockSpec(memory_space=pl.ANY)
    buffer = pltpu.VMEM((mine, peers, capacity, dim), BF16)
    sems = pltpu.SemaphoreType.DMA((mine, peers))
    return pl.pallas_call(
        functools.partial(moe_kernel, layer, axis),
        in_specs=[near] * 4 + [hbm] * 4,
        out_specs=near,
        out_shape=jax.ShapeDtypeStruct(h1.shape, BF16),
        scratch_shapes=[pltpu.VMEM(h1.shape, BF16), pltpu.VMEM(h1.shape, BF16), buffer, buffer, buffer, pltpu.VMEM((2, dim, ff), BF16), pltpu.VMEM((2, ff, dim), BF16),
                        pltpu.VMEM((rows, dim), F32), pltpu.VMEM((num_seqs, seq_len, dim), BF16),
                        pltpu.VMEM((num_seqs, seq_len, 1), jnp.int32), pltpu.VMEM((num_seqs, seq_len, 1), F32),
                        sems, sems, sems, sems, pltpu.SemaphoreType.DMA((2, 2)), pltpu.SemaphoreType.DMA((2,))],
        compiler_params=pltpu.CompilerParams(collective_id=layer, has_side_effects=True, vmem_limit_bytes=67043328),
        cost_estimate=pl.CostEstimate(flops=4 * mine * rows * dim * ff, bytes_accessed=48 << 20, transcendentals=0),
        name="moe",
    )(pos, ids, gains, w_router_t, b, h1, w_in, w_out)


def out_kernel(x_hbm, out_hbm, buf, sems):
    load = lambda i: pltpu.make_async_copy(x_hbm.at[i], buf.at[i], sems.at[0, i])
    store = lambda i: pltpu.make_async_copy(buf.at[i], out_hbm.at[i], sems.at[1, i])
    for i in range(buf.shape[0]):
        load(i).start()
    for i in range(buf.shape[0]):
        load(i).wait()
        store(i).start()
    for i in range(buf.shape[0]):
        store(i).wait()


def hand_out(x):
    hbm = pl.BlockSpec(memory_space=pl.ANY)
    return pl.pallas_call(
        out_kernel, in_specs=[hbm], out_specs=hbm, out_shape=jax.ShapeDtypeStruct(x.shape, x.dtype),
        scratch_shapes=[pltpu.VMEM(x.shape, x.dtype), pltpu.SemaphoreType.DMA((2, x.shape[0]))], name="out",
    )(x)


def solution(mesh):
    token_spec = P(('dp', 'ep'))
    peers = mesh.shape['ep']

    def per_device(x_in, pad_mask, rel_bias, expert_idx, norm_scale, w_query, w_key, w_value, w_attn_out, w_router, w_in, w_out):
        num_seqs, seq_len, model_dim = x_in.shape
        tok_count = num_seqs * seq_len
        layers = w_router.shape[0]
        num_experts = w_router.shape[2]
        mine = num_experts // peers
        capacity = (CAP_FACTOR * tok_count + num_experts - 1) // num_experts
        ids = jnp.swapaxes(expert_idx, 0, 1)
        pos = pl.pallas_call(
            functools.partial(slots_kernel, capacity, mine, num_experts),
            out_shape=jax.ShapeDtypeStruct(ids.shape, jnp.int32),
            name="slots",
        )(ids)
        w_router_t = jnp.swapaxes(w_router, 1, 2)
        hidden = x_in
        for layer in range(layers):
            h1, b = attention(layer, hidden, pad_mask, rel_bias, norm_scale, w_query, w_key, w_value, w_attn_out)
            hidden = moe(layer, 'ep', peers, capacity, pos, ids, norm_scale, w_router_t, h1, b, w_in, w_out)
        return hand_out(hidden)

    return jax.shard_map(per_device, mesh=mesh, in_specs=(token_spec, token_spec, P(), P(None, ('dp', 'ep')), P(), P(), P(), P(), P(), P(), P(None, 'ep'), P(None, 'ep')), out_specs=token_spec, check_vma=False)
```
